32 devices in a mesh: gx: 4 (over y, x), gy: 2 (over core), gz: 4 (over z).
Axes of the slice: x: 2, y: 2, z: 4, core: 2. Of those that a mesh axis runs over, the one named last changes fastest.
Arguments:
- gradient: float32 [4, 2, 4, 16, 512], P('gx', 'gy', 'gz'), may hold values from -60 to 60
- local_schur: bfloat16 [4, 2, 4, 2048, 2048], P('gx', 'gy', 'gz'), may hold values from -1 to 4
- inverse_rows: bfloat16 [4, 2, 4, 512, 2048], P('gx', 'gy', 'gz'), may hold values from -0.1 to 0.6
- face_maps: int32 [4, 2, 4, 6, 256], P('gx', 'gy', 'gz'), may hold values from 0 to 511, as said below
Outputs:
- adjoint: float32 [4, 2, 4, 16, 512], P('gx', 'gy', 'gz')
- residual_ratio: float32 [16], replicated
The draws below stay inside these ranges and needn't reach their ends.
Inputs may be any that keep to these rules, and one draw needn't show every extreme that they name: `face_maps`: for each subdomain and face, 256 distinct owned rows of the neighbour across that face.
All inputs are finite; a program needn't handle non-finite values.
Results may differ from the reference program's by a relative error of at most 0.0038.
Values may be sent and summed in bfloat16 or wider, within the bound.
A program may use at most 64 MiB of HBM per device.

```python
import math
import jax
import jax.numpy as jnp
from jax import lax

M = 2048
OWN = 512
RHS = 16
ITERS = 3
FACE = 256
SX = 4
SY = 2
SZ = 4


def device_ramp(highest):
    devices_n = SX * SY * SZ
    flat_ids = jnp.arange(devices_n, dtype=jnp.float32).reshape(SX, SY, SZ, 1, 1)
    return 1.0 + (highest - 1.0) * flat_ids / max(devices_n - 1, 1)


def draw_gradient(key, part):
    subkeys = jax.random.split(jax.random.fold_in(key, 11), 3)
    shape = (SX, SY, SZ, RHS, OWN)
    row_scale = jnp.exp(jax.random.uniform(subkeys[1], (SX, SY, SZ, 1, OWN), jnp.float32, math.log(0.3), math.log(3.0)))
    rhs_scale = jnp.exp(jax.random.uniform(subkeys[2], (1, 1, 1, RHS, 1), jnp.float32, math.log(0.5), math.log(1.5)))
    base_vals = jnp.clip(jax.random.normal(subkeys[0], shape, jnp.float32), -4.0, 4.0)
    ramp_vals = device_ramp(3.0)
    return base_vals * row_scale * rhs_scale * ramp_vals


def draw_local_schur(key, part):
    subkeys = jax.random.split(jax.random.fold_in(key, 23), 2)
    shape = (SX, SY, SZ, M, M)
    sigma = 0.6 / math.sqrt(M)
    noise = jnp.clip(jax.random.normal(subkeys[0], shape, jnp.float32), -4.0, 4.0) * sigma
    diagonal = jax.random.uniform(subkeys[1], (SX, SY, SZ, 1, M), jnp.float32, 1.0, 3.0)
    identity = (jnp.arange(M)[:, None] == jnp.arange(M)[None, :]).astype(jnp.float32)
    return (noise + diagonal * identity).astype(jnp.bfloat16)


def draw_inverse_rows(key, part):
    subkeys = jax.random.split(jax.random.fold_in(key, 37), 2)
    shape = (SX, SY, SZ, OWN, M)
    sigma = 0.1 / math.sqrt(M)
    noise = jnp.clip(jax.random.normal(subkeys[0], shape, jnp.float32), -4.0, 4.0) * sigma
    diagonal = jnp.exp(jax.random.uniform(subkeys[1], (SX, SY, SZ, OWN, 1), jnp.float32, math.log(0.1), math.log(0.5)))
    identity = (jnp.arange(OWN)[:, None] == jnp.arange(M)[None, :]).astype(jnp.float32)
    return (noise + diagonal * identity).astype(jnp.bfloat16)


def draw_face_maps(key, part):
    scores = jax.random.randint(jax.random.fold_in(key, 53), (SX, SY, SZ, 6, OWN), 0, 1 << 20, jnp.int32)
    scores = scores * OWN + jnp.arange(OWN, dtype=jnp.int32)
    return jnp.argsort(scores, axis=-1)[..., :FACE].astype(jnp.int32)


def setup_inputs(seed: int = 0) -> dict:
    streams_of = jax.random.split(jax.random.key(seed), 5)
    gradient = draw_gradient(jax.random.fold_in(streams_of[4], 71), 0)
    local_schur = draw_local_schur(jax.random.fold_in(streams_of[4], 71), 0)
    inverse_rows = draw_inverse_rows(jax.random.fold_in(streams_of[4], 71), 0)
    face_maps = draw_face_maps(jax.random.fold_in(streams_of[4], 71), 0)
    return {"gradient": gradient, "local_schur": local_schur, "inverse_rows": inverse_rows, "face_maps": face_maps}


EPSILON = 1e-06

def across(values, facing):
    dimension = facing // 2
    widths = [(0, 0)] * values.ndim
    extent = values.shape[dimension]
    if facing % 2 == 0:
        widths[dimension] = (1, 0)
        return lax.slice_in_dim(jnp.pad(values, widths), 0, extent, axis=dimension)
    widths[dimension] = (0, 1)
    return lax.slice_in_dim(jnp.pad(values, widths), 1, extent + 1, axis=dimension)

def flatten_grid(values):
    return values.reshape((-1,) + values.shape[3:])

def take_rows(face_block, row_ids):
    return jnp.take(face_block, row_ids, axis=1)

def add_rows(face_block, row_ids, addition):
    return face_block.at[:, row_ids].add(addition)

def multiply_pair(operands):
    return jnp.dot(operands[0], operands[1], preferred_element_type=jnp.float32)

def assemble(products, face_maps):
    owned = products.shape[-1] - 6 * FACE
    result = flatten_grid(products[..., :owned])
    for facing in range(6):
        offset = owned + (facing ^ 1) * FACE
        face_block = across(products[..., offset:offset + FACE], facing)
        row_ids = across(face_maps[..., facing ^ 1, :], facing)
        result = jax.vmap(add_rows)(result, flatten_grid(row_ids), flatten_grid(face_block))
    return result.reshape(products.shape[:-1] + (owned,))

def operator(values, face_maps, local_schur):
    rounded = values.astype(jnp.bfloat16)
    ghosts = [jax.vmap(take_rows)(flatten_grid(across(rounded, facing)), flatten_grid(face_maps[..., facing, :])) for facing in range(6)]
    intersected = jnp.concatenate([flatten_grid(rounded)] + ghosts, axis=2)
    products = lax.map(multiply_pair, (intersected, flatten_grid(local_schur)))
    return assemble(products.reshape(values.shape[:3] + products.shape[1:]), face_maps)

def precondition(values, face_maps, inverse_rows):
    rounded = flatten_grid(values.astype(jnp.bfloat16))
    products = lax.map(multiply_pair, (rounded, flatten_grid(inverse_rows)))
    return assemble(products.reshape(values.shape[:3] + products.shape[1:]), face_maps)

def inner_sum(left_side, right_side):
    return lax.optimization_barrier(jnp.sum(left_side * right_side, axis=(0, 1, 2, 4)))

def rotate_solve(columns, beta_norm):
    num_cols = len(columns)
    rhs_vec = [beta_norm] + [jnp.zeros_like(beta_norm) for unused in range(num_cols)]
    cosines = []
    sines = []
    triangle = []
    for section in range(num_cols):
        column = [columns[section][row_at] for row_at in range(section + 2)]
        for earlier in range(section):
            rotated_a = cosines[earlier] * column[earlier] + sines[earlier] * column[earlier + 1]
            rotated_b = -sines[earlier] * column[earlier] + cosines[earlier] * column[earlier + 1]
            column[earlier] = rotated_a
            column[earlier + 1] = rotated_b
        radius = jnp.sqrt(column[section] * column[section] + column[section + 1] * column[section + 1])
        cosine = column[section] / radius
        sine_val = column[section + 1] / radius
        column[section] = radius
        cosines.append(cosine)
        sines.append(sine_val)
        rhs_vec[section + 1] = -sine_val * rhs_vec[section]
        rhs_vec[section] = cosine * rhs_vec[section]
        triangle.append(column[:section + 1])
    coeffs = [None] * num_cols
    for section in reversed(range(num_cols)):
        running = rhs_vec[section]
        for onward in range(section + 1, num_cols):
            running = running - triangle[onward][section] * coeffs[onward]
        coeffs[section] = running / triangle[section][section]
    return (coeffs, jnp.abs(rhs_vec[num_cols]))

def reference(gradient, local_schur, inverse_rows, face_maps):
    beta_norm = jnp.sqrt(inner_sum(gradient, gradient) + EPSILON)
    krylov = [gradient / beta_norm[:, None]]
    directions = []
    columns = []
    for section in range(ITERS):
        prepared = precondition(krylov[section], face_maps, inverse_rows)
        directions.append(prepared)
        applied = operator(prepared, face_maps, local_schur)
        coeffs = [inner_sum(vector, applied) for vector in krylov]
        residue = applied
        for position in range(section + 1):
            residue = residue - coeffs[position][:, None] * krylov[position]
        height = jnp.sqrt(inner_sum(residue, residue) + EPSILON)
        columns.append(coeffs + [height])
        if section + 1 < ITERS:
            krylov.append(residue / height[:, None])
    weights, remainder = rotate_solve(columns, beta_norm)
    adjoint = weights[0][:, None] * directions[0]
    for position in range(1, ITERS):
        adjoint = adjoint + weights[position][:, None] * directions[position]
    return (adjoint, remainder / beta_norm)
```

```python
import functools

import jax
import jax.numpy as jnp
from jax import lax
from jax.experimental import pallas as pl
from jax.experimental.pallas import tpu as pltpu
from jax.sharding import PartitionSpec as P

ITERS = 3
EPSILON = 1e-06
FACE_ORDER = (0, 1, 4, 5, 2, 3)
MESH = pl.DeviceIdType.MESH
BF16 = jnp.bfloat16
F32 = jnp.float32


def split(x):
    high = x.astype(BF16)
    low = (x - high.astype(F32)).astype(BF16)
    return jnp.concatenate([high, low], axis=0)


def merge(x):
    rows = x.shape[0] // 2
    return x[:rows] + x[rows:]


def mm(a, b):
    return jnp.dot(a, b, preferred_element_type=F32)


def rotate_solve(columns, beta_norm):
    num_cols = len(columns)
    rhs_vec = [beta_norm] + [jnp.zeros_like(beta_norm) for unused in range(num_cols)]
    cosines = []
    sines = []
    triangle = []
    for section in range(num_cols):
        column = [columns[section][row_at] for row_at in range(section + 2)]
        for earlier in range(section):
            rotated_a = cosines[earlier] * column[earlier] + sines[earlier] * column[earlier + 1]
            rotated_b = -sines[earlier] * column[earlier] + cosines[earlier] * column[earlier + 1]
            column[earlier] = rotated_a
            column[earlier + 1] = rotated_b
        radius = jnp.sqrt(
            column[section] * column[section] + column[section + 1] * column[section + 1]
        )
        cosine = column[section] / radius
        sine_val = column[section + 1] / radius
        column[section] = radius
        cosines.append(cosine)
        sines.append(sine_val)
        rhs_vec[section + 1] = -sine_val * rhs_vec[section]
        rhs_vec[section] = cosine * rhs_vec[section]
        triangle.append(column[: section + 1])
    coeffs = [None] * num_cols
    for section in reversed(range(num_cols)):
        running = rhs_vec[section]
        for onward in range(section + 1, num_cols):
            running = running - triangle[onward][section] * coeffs[onward]
        coeffs[section] = running / triangle[section][section]
    return (coeffs, jnp.abs(rhs_vec[num_cols]))


def kernel(
    sizes, g_ref, maps_ref, k_hbm, b_hbm, out_ref, ratio_ref,
    k_ref, b_ref, near_maps, gather_ref, scatter_ref, send_buf, recv_buf, acc_ref,
    t_ref, v_ref, z_ref, w_ref, last_ref, total_ref, plane_buf, line_buf,
    weight_sem, map_send, map_recv, send_sem, recv_sem,
    plane_send, plane_recv, line_send, line_recv,
):
    nx, ny, nz = sizes
    rhs, own = g_ref.shape
    face = maps_ref.shape[1]
    ix, iy, iz = lax.axis_index("gx"), lax.axis_index("gy"), lax.axis_index("gz")
    spots = ((ix, nx), (ix, nx), (iy, ny), (iy, ny), (iz, nz), (iz, nz))
    exists = [
        spots[f][0] > 0 if f % 2 == 0 else spots[f][0] < spots[f][1] - 1 for f in range(6)
    ]

    def across(f):
        step = 2 * (f % 2) - 1
        place = [ix, iy, iz]
        place[f // 2] = place[f // 2] + step
        return tuple(place)

    faces = [f for f in FACE_ORDER if spots[f][1] > 1]
    plane = [
        (lax.rem(ix + dx, nx), lax.rem(iy + dy, ny))
        for dx in range(nx) for dy in range(ny) if dx or dy
    ]
    line = [lax.rem(iz + dz, nz) for dz in range(1, nz)]

    weights = [pltpu.make_async_copy(b_hbm, b_ref, weight_sem.at[0])]
    weights.append(
        pltpu.make_async_copy(k_hbm.at[pl.ds(0, own)], k_ref.at[pl.ds(0, own)], weight_sem.at[1])
    )
    ghosts = pl.ds(own, k_ref.shape[0] - own)
    weights.append(pltpu.make_async_copy(k_hbm.at[ghosts], k_ref.at[ghosts], weight_sem.at[2]))
    for copy in weights:
        copy.start()

    barrier = pltpu.get_barrier_semaphore()
    for px, py in plane:
        pl.semaphore_signal(barrier, inc=1, device_id=(px, py, iz), device_id_type=MESH)
    for pz in line:
        pl.semaphore_signal(barrier, inc=1, device_id=(ix, iy, pz), device_id_type=MESH)

    t_ref[...] = g_ref[...]
    v_ref[...] = jnp.zeros_like(v_ref)
    z_ref[...] = jnp.zeros_like(z_ref)
    w_ref[...] = jnp.zeros_like(w_ref)
    last_ref[...] = jnp.zeros_like(last_ref)
    total_ref[...] = jnp.zeros_like(total_ref)
    for f in range(6):
        @pl.when(jnp.logical_not(exists[f]))
        def _():
            near_maps[f] = jnp.full(near_maps.shape[1:], -1, jnp.int32)
            for e in range(3 * ITERS):
                recv_buf[e, f] = jnp.zeros(recv_buf.shape[2:], BF16)

    pl.semaphore_wait(barrier, len(plane) + len(line))

    def map_copy(f, slot):
        return pltpu.make_async_remote_copy(
            src_ref=maps_ref, dst_ref=near_maps.at[slot], send_sem=map_send.at[f],
            recv_sem=map_recv.at[slot], device_id=across(f), device_id_type=MESH,
        )

    def face_copy(e, f, slot):
        return pltpu.make_async_remote_copy(
            src_ref=send_buf.at[e, f], dst_ref=recv_buf.at[e, slot], send_sem=send_sem.at[e, f],
            recv_sem=recv_sem.at[e, slot], device_id=across(f), device_id_type=MESH,
        )

    def plane_copy(r, peer, slot):
        mine = ix * ny + iy
        return pltpu.make_async_remote_copy(
            src_ref=plane_buf.at[r, mine], dst_ref=plane_buf.at[r, slot],
            send_sem=plane_send.at[r, peer[0] * ny + peer[1]], recv_sem=plane_recv.at[r, slot],
            device_id=(peer[0], peer[1], iz), device_id_type=MESH,
        )

    def line_copy(r, peer, slot):
        return pltpu.make_async_remote_copy(
            src_ref=line_buf.at[r, iz], dst_ref=line_buf.at[r, slot],
            send_sem=line_send.at[r, peer], recv_sem=line_recv.at[r, slot],
            device_id=(ix, iy, peer), device_id_type=MESH,
        )

    for f in faces:
        @pl.when(exists[f])
        def _():
            map_copy(f, f ^ 1).start()

    lanes = lax.broadcasted_iota(jnp.int32, (rhs, 128), 1)
    half = rhs // 2

    def start_sums(r):
        t = t_ref[...]
        last = last_ref[...]
        packed = jnp.where(lanes == ITERS, jnp.sum(t * t, axis=1, keepdims=True), 0.0)
        for k in range(ITERS):
            v = v_ref[k]
            packed = jnp.where(lanes == k, jnp.sum(v * t, axis=1, keepdims=True), packed)
            packed = jnp.where(
                lanes == ITERS + 1 + k, jnp.sum(v * last, axis=1, keepdims=True), packed
            )
        plane_buf[r, ix * ny + iy] = packed[:half] + pltpu.roll(packed[half:], 64, 1)
        for peer in plane:
            plane_copy(r, peer, ix * ny + iy).start()

    def pass_sums(r):
        for peer in plane:
            plane_copy(r, peer, peer[0] * ny + peer[1]).wait_recv()
        partial = plane_buf[r, 0]
        for at in range(1, nx * ny):
            partial = partial + plane_buf[r, at]
        line_buf[r, iz] = partial
        for peer in line:
            line_copy(r, peer, iz).start()

    def finish_sums(r):
        for peer in line:
            line_copy(r, peer, peer).wait_recv()
        total = line_buf[r, 0]
        for at in range(1, nz):
            total = total + line_buf[r, at]
        total_ref[r] = jnp.concatenate([total, pltpu.roll(total, 64, 1)], axis=0)

    def pick(r, lane):
        return jnp.sum(jnp.where(lanes == lane, total_ref[r], 0.0), axis=1, keepdims=True)

    def heights(r, count):
        coeffs = [pick(r, k) for k in range(count)]
        running = pick(r, ITERS)
        for k in range(count):
            running = running - 2.0 * coeffs[k] * coeffs[k]
            for n in range(k + 1):
                element = coeffs[k] * pick(k + 1, ITERS + 1 + n) * coeffs[n]
                running = running + (element if n == k else 2.0 * element)
        return coeffs, jnp.sqrt(jnp.maximum(running, 0.0) + EPSILON)

    def block(f):
        return pl.ds(own + f * face, face)

    def scattered(e, base):
        for f in faces:
            @pl.when(exists[f])
            def _():
                face_copy(e, f, f).wait_recv()
        added = mm(recv_buf[e, faces[0]], scatter_ref[faces[0]])
        for f in faces[1:]:
            added = added + mm(recv_buf[e, f], scatter_ref[f])
        return base + merge(added)

    def send(e, f, pair):
        send_buf[e, f] = pair

        @pl.when(exists[f])
        def _():
            face_copy(e, f, f ^ 1).start()

    def iteration(j, carry):
        first, second, third = 3 * j, 3 * j + 1, 3 * j + 2
        pair = split(t_ref[...])

        @pl.when(j == 0)
        def _():
            weights[0].wait()

        for f in faces:
            send(first, f, split(merge(mm(pair, b_ref[:, block(f)]))))
        start_sums(j)
        base = merge(mm(pair, b_ref[:, pl.ds(0, own)]))

        @pl.when(j == 0)
        def _():
            for f in faces:
                @pl.when(exists[f])
                def _():
                    map_copy(f, f).wait_recv()
            for f in faces:
                row = near_maps[f, pl.ds(f ^ 1, 1), :]
                hot = lax.broadcasted_iota(jnp.int32, (own, face), 0) == row
                hot = jnp.where(hot, 1.0, 0.0)
                gather_ref[f] = hot.astype(BF16)
                scatter_ref[f] = jnp.transpose(hot).astype(BF16)

        prepared = scattered(first, base)
        pair = split(prepared)
        for f in faces:
            send(second, f, mm(pair, gather_ref[f]).astype(BF16))
        pass_sums(j)

        @pl.when(j == 0)
        def _():
            weights[1].wait()

        acc_ref[...] = mm(pair, k_ref[pl.ds(0, own), :])

        @pl.when(j == 0)
        def _():
            weights[2].wait()

        for f in faces:
            @pl.when(exists[f])
            def _():
                face_copy(second, f, f).wait_recv()
        left = jnp.concatenate([recv_buf[second, f] for f in range(6)], axis=1)
        for f in faces:
            product = acc_ref[:, block(f)] + mm(left, k_ref[ghosts, block(f)])
            send(third, f, split(merge(product)))
        base = merge(acc_ref[:, pl.ds(0, own)] + mm(left, k_ref[ghosts, pl.ds(0, own)]))
        finish_sums(j)
        coeffs, height = heights(j, ITERS - 1)
        inverse = 1.0 / height
        newest = t_ref[...]
        for k in range(ITERS - 1):
            prepared = prepared - coeffs[k] * z_ref[k]
            newest = newest - coeffs[k] * v_ref[k]
        z_ref[j] = prepared * inverse
        newest = newest * inverse
        v_ref[j] = newest
        last_ref[...] = newest
        applied = scattered(third, base)
        for k in range(ITERS - 1):
            applied = applied - coeffs[k] * w_ref[k]
        applied = applied * inverse
        w_ref[j] = applied
        t_ref[...] = applied
        return carry

    lax.fori_loop(0, ITERS, iteration, 0)
    start_sums(ITERS)
    pass_sums(ITERS)
    finish_sums(ITERS)
    beta_norm = heights(0, 0)[1]
    columns = []
    for section in range(ITERS):
        coeffs, height = heights(section + 1, section + 1)
        columns.append(coeffs + [height])
    solved, remainder = rotate_solve(columns, beta_norm)
    adjoint = solved[0] * z_ref[0]
    for k in range(1, ITERS):
        adjoint = adjoint + solved[k] * z_ref[k]
    out_ref[...] = adjoint
    rows = lax.broadcasted_iota(jnp.int32, (rhs, 128), 0)
    spread = jnp.where(rows == lanes, remainder / beta_norm, 0.0)
    ratio_ref[...] = jnp.sum(spread, axis=0, keepdims=True)[:, :rhs]

    for f in faces:
        @pl.when(exists[f])
        def _():
            map_copy(f, f ^ 1).wait_send()
            for e in range(3 * ITERS):
                face_copy(e, f, f ^ 1).wait_send()
    for r in range(ITERS + 1):
        for peer in plane:
            plane_copy(r, peer, ix * ny + iy).wait_send()
        for peer in line:
            line_copy(r, peer, iz).wait_send()


def local(sizes, gradient, local_schur, inverse_rows, face_maps):
    nx, ny, nz = sizes
    target = gradient[0, 0, 0]
    rhs, own = target.shape
    maps = face_maps[0, 0, 0]
    face = maps.shape[1]
    whole = local_schur.shape[-1]
    exchanges = 3 * ITERS
    sums = ITERS + 1
    vmem = pl.BlockSpec(memory_space=pltpu.VMEM)
    hbm = pl.BlockSpec(memory_space=pl.ANY)
    dma = pltpu.SemaphoreType.DMA
    adjoint, ratio = pl.pallas_call(
        functools.partial(kernel, sizes),
        out_shape=(
            jax.ShapeDtypeStruct((rhs, own), F32),
            jax.ShapeDtypeStruct((1, rhs), F32),
        ),
        in_specs=[vmem, vmem, hbm, hbm],
        out_specs=(vmem, vmem),
        scratch_shapes=[
            pltpu.VMEM((whole, whole), BF16),
            pltpu.VMEM((own, whole), BF16),
            pltpu.VMEM((6,) + maps.shape, jnp.int32),
            pltpu.VMEM((6, own, face), BF16),
            pltpu.VMEM((6, face, own), BF16),
            pltpu.VMEM((exchanges, 6, 2 * rhs, face), BF16),
            pltpu.VMEM((exchanges, 6, 2 * rhs, face), BF16),
            pltpu.VMEM((2 * rhs, whole), F32),
            pltpu.VMEM((rhs, own), F32),
            pltpu.VMEM((ITERS, rhs, own), F32),
            pltpu.VMEM((ITERS, rhs, own), F32),
            pltpu.VMEM((ITERS, rhs, own), F32),
            pltpu.VMEM((rhs, own), F32),
            pltpu.VMEM((sums, rhs, 128), F32),
            pltpu.VMEM((sums, nx * ny, rhs // 2, 128), F32),
            pltpu.VMEM((sums, nz, rhs // 2, 128), F32),
            dma((3,)),
            dma((6,)),
            dma((6,)),
            dma((exchanges, 6)),
            dma((exchanges, 6)),
            dma((sums, nx * ny)),
            dma((sums, nx * ny)),
            dma((sums, nz)),
            dma((sums, nz)),
        ],
        compiler_params=pltpu.CompilerParams(
            collective_id=0, has_side_effects=True, vmem_limit_bytes=56 * 1024 * 1024
        ),
    )(target, maps, local_schur[0, 0, 0], inverse_rows[0, 0, 0])
    return (adjoint[None, None, None], ratio[0])


def solution(mesh):
    placed = P("gx", "gy", "gz", None, None)
    sizes = (mesh.shape["gx"], mesh.shape["gy"], mesh.shape["gz"])
    return jax.shard_map(
        functools.partial(local, sizes),
        mesh=mesh,
        in_specs=(placed, placed, placed, placed),
        out_specs=(placed, P()),
        check_vma=False,
    )
```

```python
import functools

import jax
import jax.numpy as jnp
from jax import lax
from jax.experimental import pallas as pl
from jax.experimental.pallas import tpu as pltpu
from jax.sharding import PartitionSpec as P

ITERS = 3
EPSILON = 1e-06
FAR = (0, 1)
NEAR = (4, 5, 2, 3)
MESH = pl.DeviceIdType.MESH
BF16 = jnp.bfloat16
F32 = jnp.float32


def split(x):
    high = x.astype(BF16)
    low = (x - high.astype(F32)).astype(BF16)
    return jnp.concatenate([high, low], axis=0)


def merge(x):
    rows = x.shape[0] // 2
    return x[:rows] + x[rows:]


def mm(a, b):
    return jnp.dot(a, b, preferred_element_type=F32)


def rotate_solve(columns, beta_norm):
    num_cols = len(columns)
    rhs_vec = [beta_norm] + [jnp.zeros_like(beta_norm) for unused in range(num_cols)]
    cosines = []
    sines = []
    triangle = []
    for section in range(num_cols):
        column = [columns[section][row_at] for row_at in range(section + 2)]
        for earlier in range(section):
            rotated_a = cosines[earlier] * column[earlier] + sines[earlier] * column[earlier + 1]
            rotated_b = -sines[earlier] * column[earlier] + cosines[earlier] * column[earlier + 1]
            column[earlier] = rotated_a
            column[earlier + 1] = rotated_b
        radius = jnp.sqrt(
            column[section] * column[section] + column[section + 1] * column[section + 1]
        )
        cosine = column[section] / radius
        sine_val = column[section + 1] / radius
        column[section] = radius
        cosines.append(cosine)
        sines.append(sine_val)
        rhs_vec[section + 1] = -sine_val * rhs_vec[section]
        rhs_vec[section] = cosine * rhs_vec[section]
        triangle.append(column[: section + 1])
    coeffs = [None] * num_cols
    for section in reversed(range(num_cols)):
        running = rhs_vec[section]
        for onward in range(section + 1, num_cols):
            running = running - triangle[onward][section] * coeffs[onward]
        coeffs[section] = running / triangle[section][section]
    return (coeffs, jnp.abs(rhs_vec[num_cols]))


def kernel(
    sizes, g_ref, maps_ref, k_hbm, b_hbm, out_ref, ratio_ref,
    k_ref, b_ref, near_maps, gather_ref, scatter_ref, send_buf, recv_buf, acc_ref,
    base_ref, t_ref, v_ref, z_ref, w_ref, last_ref, total_ref, plane_buf, line_buf,
    weight_sem, map_send, map_recv, send_sem, recv_sem,
    plane_send, plane_recv, line_send, line_recv,
):
    nx, ny, nz = sizes
    rhs, own = g_ref.shape
    face = maps_ref.shape[-1]
    ix, iy, iz = lax.axis_index("gx"), lax.axis_index("gy"), lax.axis_index("gz")
    spots = ((ix, nx), (ix, nx), (iy, ny), (iy, ny), (iz, nz), (iz, nz))
    exists = [
        spots[f][0] > 0 if f % 2 == 0 else spots[f][0] < spots[f][1] - 1 for f in range(6)
    ]

    def across(f):
        step = 2 * (f % 2) - 1
        place = [ix, iy, iz]
        place[f // 2] = place[f // 2] + step
        return tuple(place)

    faces = [f for f in FAR + NEAR if spots[f][1] > 1]
    far_width, near_width = len(FAR) * face, len(NEAR) * face
    far_columns = pl.ds(own, far_width)
    near_columns = pl.ds(own + far_width, near_width)
    plane = [
        (lax.rem(ix + dx, nx), lax.rem(iy + dy, ny))
        for dx in range(nx) for dy in range(ny) if dx or dy
    ]
    line = [lax.rem(iz + dz, nz) for dz in range(1, nz)]

    weights = [pltpu.make_async_copy(b_hbm, b_ref, weight_sem.at[0])]
    weights.append(
        pltpu.make_async_copy(k_hbm.at[pl.ds(0, own)], k_ref.at[pl.ds(0, own)], weight_sem.at[1])
    )
    ghosts = pl.ds(own, k_ref.shape[0] - own)
    weights.append(pltpu.make_async_copy(k_hbm.at[ghosts], k_ref.at[ghosts], weight_sem.at[2]))
    for copy in weights:
        copy.start()

    barrier = pltpu.get_barrier_semaphore()
    for px, py in plane:
        pl.semaphore_signal(barrier, inc=1, device_id=(px, py, iz), device_id_type=MESH)
    for pz in line:
        pl.semaphore_signal(barrier, inc=1, device_id=(ix, iy, pz), device_id_type=MESH)

    t_ref[...] = g_ref[...]
    v_ref[...] = jnp.zeros_like(v_ref)
    z_ref[...] = jnp.zeros_like(z_ref)
    w_ref[...] = jnp.zeros_like(w_ref)
    last_ref[...] = jnp.zeros_like(last_ref)
    total_ref[...] = jnp.zeros_like(total_ref)
    for f in range(6):
        @pl.when(jnp.logical_not(exists[f]))
        def _():
            near_maps[f] = jnp.full(near_maps.shape[1:], -1, jnp.int32)
            for e in range(3 * ITERS):
                recv_buf[e, f] = jnp.zeros(recv_buf.shape[2:], BF16)

    def map_copy(f, slot):
        return pltpu.make_async_remote_copy(
            src_ref=maps_ref, dst_ref=near_maps.at[slot], send_sem=map_send.at[f],
            recv_sem=map_recv.at[slot], device_id=across(f), device_id_type=MESH,
        )

    def face_copy(e, f, slot):
        return pltpu.make_async_remote_copy(
            src_ref=send_buf.at[e, f], dst_ref=recv_buf.at[e, slot], send_sem=send_sem.at[e, f],
            recv_sem=recv_sem.at[e, slot], device_id=across(f), device_id_type=MESH,
        )

    def plane_copy(r, peer, slot):
        mine = ix * ny + iy
        return pltpu.make_async_remote_copy(
            src_ref=plane_buf.at[r, mine], dst_ref=plane_buf.at[r, slot],
            send_sem=plane_send.at[r, peer[0] * ny + peer[1]], recv_sem=plane_recv.at[r, slot],
            device_id=(peer[0], peer[1], iz), device_id_type=MESH,
        )

    def line_copy(r, peer, slot):
        return pltpu.make_async_remote_copy(
            src_ref=line_buf.at[r, iz], dst_ref=line_buf.at[r, slot],
            send_sem=line_send.at[r, peer], recv_sem=line_recv.at[r, slot],
            device_id=(ix, iy, peer), device_id_type=MESH,
        )

    lanes = lax.broadcasted_iota(jnp.int32, (rhs, 128), 1)
    rows = lax.broadcasted_iota(jnp.int32, (rhs, 128), 0)
    group = 128 // rhs
    places = lax.rem(lanes, group)
    mine = lax.div(lanes, group) == rows

    def start_sums(r):
        t = t_ref[...]
        last = last_ref[...]
        packed = jnp.where(places == ITERS, jnp.sum(t * t, axis=1, keepdims=True), 0.0)
        for k in range(ITERS):
            v = v_ref[k]
            packed = jnp.where(places == k, jnp.sum(v * t, axis=1, keepdims=True), packed)
            packed = jnp.where(
                places == ITERS + 1 + k, jnp.sum(v * last, axis=1, keepdims=True), packed
            )
        packed = jnp.where(mine, packed, 0.0)
        plane_buf[r, ix * ny + iy] = jnp.sum(packed, axis=0, keepdims=True)
        for peer in plane:
            plane_copy(r, peer, ix * ny + iy).start()

    def pass_sums(r):
        for peer in plane:
            plane_copy(r, peer, peer[0] * ny + peer[1]).wait_recv()
        partial = plane_buf[r, 0]
        for at in range(1, nx * ny):
            partial = partial + plane_buf[r, at]
        line_buf[r, iz] = partial
        for peer in line:
            line_copy(r, peer, iz).start()

    def finish_sums(r):
        for peer in line:
            line_copy(r, peer, peer).wait_recv()
        total = line_buf[r, 0]
        for at in range(1, nz):
            total = total + line_buf[r, at]
        total_ref[r] = jnp.where(mine, total, 0.0)

    def pick(r, lane):
        return jnp.sum(jnp.where(places == lane, total_ref[r], 0.0), axis=1, keepdims=True)

    def heights(r, count):
        coeffs = [pick(r, k) for k in range(count)]
        running = pick(r, ITERS)
        for k in range(count):
            running = running - 2.0 * coeffs[k] * coeffs[k]
            for n in range(k + 1):
                element = coeffs[k] * pick(k + 1, ITERS + 1 + n) * coeffs[n]
                running = running + (element if n == k else 2.0 * element)
        return coeffs, jnp.sqrt(jnp.maximum(running, 0.0) + EPSILON)

    def arrived(e, group):
        for f in group:
            if f in faces:
                @pl.when(exists[f])
                def _():
                    face_copy(e, f, f).wait_recv()
        return jnp.concatenate([recv_buf[e, f] for f in sorted(group)], axis=1)

    def scattered(e, base):
        added = mm(arrived(e, NEAR), scatter_ref[pl.ds(far_width, near_width), :])
        added = added + mm(arrived(e, FAR), scatter_ref[pl.ds(0, far_width), :])
        return base + merge(added)

    def stage(e, group, pairs):
        for at, f in enumerate(sorted(group)):
            send_buf[e, f] = pairs[:, at * face : (at + 1) * face]

    def send(e, group):
        odd = lax.rem(ix, 2) == 1

        def start(f, when):
            if f in faces:
                @pl.when(jnp.logical_and(exists[f], when))
                def _():
                    face_copy(e, f, f ^ 1).start()

        if group is FAR:
            start(1, odd)
            start(0, True)
            start(1, jnp.logical_not(odd))
        else:
            for f in group:
                start(f, True)

    def precondition(e, ready):
        pair = split(t_ref[...])
        stage(e, FAR, split(merge(mm(pair, b_ref[:, far_columns]))))
        ready()
        send(e, FAR)
        stage(e, NEAR, split(merge(mm(pair, b_ref[:, near_columns]))))
        send(e, NEAR)
        base_ref[...] = merge(mm(pair, b_ref[:, pl.ds(0, own)]))

    def iteration(j, carry):
        first, second, third = 3 * j, 3 * j + 1, 3 * j + 2
        start_sums(j)

        @pl.when(j == 0)
        def _():
            for f in faces:
                @pl.when(exists[f])
                def _():
                    map_copy(f, f).wait_recv()
            for f in range(6):
                row = near_maps[f, f ^ 1]
                hot = lax.broadcasted_iota(jnp.int32, (own, face), 0) == row
                hot = jnp.where(hot, 1.0, 0.0)
                gather_ref[:, pl.ds(f * face, face)] = hot.astype(BF16)
                scatter_ref[pl.ds(f * face, face), :] = jnp.transpose(hot).astype(BF16)

        prepared = scattered(first, base_ref[...])
        pair = split(prepared)
        stage(second, FAR, mm(pair, gather_ref[:, pl.ds(0, far_width)]).astype(BF16))
        send(second, FAR)
        stage(second, NEAR, mm(pair, gather_ref[:, pl.ds(far_width, near_width)]).astype(BF16))
        send(second, NEAR)
        pass_sums(j)

        @pl.when(j == 0)
        def _():
            weights[1].wait()

        acc_ref[...] = mm(pair, k_ref[pl.ds(0, own), :])

        @pl.when(j == 0)
        def _():
            weights[2].wait()

        acc_ref[...] += mm(arrived(second, NEAR), k_ref[near_columns, :])
        left = arrived(second, FAR)

        def products(columns):
            return merge(acc_ref[:, columns] + mm(left, k_ref[far_columns, columns]))

        stage(third, FAR, split(products(far_columns)))
        send(third, FAR)
        stage(third, NEAR, split(products(near_columns)))
        send(third, NEAR)
        base = products(pl.ds(0, own))
        finish_sums(j)
        coeffs, height = heights(j, ITERS - 1)
        inverse = 1.0 / height
        newest = t_ref[...]
        for k in range(ITERS - 1):
            prepared = prepared - coeffs[k] * z_ref[k]
            newest = newest - coeffs[k] * v_ref[k]
        z_ref[j] = prepared * inverse
        newest = newest * inverse
        v_ref[j] = newest
        last_ref[...] = newest
        applied = scattered(third, base)
        for k in range(ITERS - 1):
            applied = applied - coeffs[k] * w_ref[k]
        applied = applied * inverse
        w_ref[j] = applied
        t_ref[...] = applied

        @pl.when(j < ITERS - 1)
        def _():
            precondition(3 * j + 3, lambda: None)

        return carry


    def ready():
        pl.semaphore_wait(barrier, len(plane) + len(line))

    weights[0].wait()
    precondition(0, ready)
    for f in faces:
        @pl.when(exists[f])
        def _():
            map_copy(f, f ^ 1).start()
    lax.fori_loop(0, ITERS, iteration, 0)
    start_sums(ITERS)
    pass_sums(ITERS)
    finish_sums(ITERS)
    beta_norm = heights(0, 0)[1]
    columns = []
    for section in range(ITERS):
        coeffs, height = heights(section + 1, section + 1)
        columns.append(coeffs + [height])
    solved, remainder = rotate_solve(columns, beta_norm)
    adjoint = solved[0] * z_ref[0]
    for k in range(1, ITERS):
        adjoint = adjoint + solved[k] * z_ref[k]
    out_ref[...] = adjoint
    spread = jnp.where(rows == lanes, remainder / beta_norm, 0.0)
    ratio_ref[...] = jnp.sum(spread, axis=0, keepdims=True)[:, :rhs]

    for f in faces:
        @pl.when(exists[f])
        def _():
            map_copy(f, f ^ 1).wait_send()
            for e in range(3 * ITERS):
                face_copy(e, f, f ^ 1).wait_send()
    for r in range(ITERS + 1):
        for peer in plane:
            plane_copy(r, peer, ix * ny + iy).wait_send()
        for peer in line:
            line_copy(r, peer, iz).wait_send()


def local(sizes, gradient, local_schur, inverse_rows, face_maps):
    nx, ny, nz = sizes
    target = gradient[0, 0, 0]
    rhs, own = target.shape
    maps = jnp.swapaxes(face_maps[0, 0], 0, 1)
    face = maps.shape[-1]
    whole = local_schur.shape[-1]
    exchanges = 3 * ITERS
    sums = ITERS + 1
    vmem = pl.BlockSpec(memory_space=pltpu.VMEM)
    hbm = pl.BlockSpec(memory_space=pl.ANY)
    dma = pltpu.SemaphoreType.DMA
    adjoint, ratio = pl.pallas_call(
        functools.partial(kernel, sizes),
        out_shape=(
            pltpu.VMEM((rhs, own), F32),
            pltpu.VMEM((1, rhs), F32),
        ),
        in_specs=[vmem, vmem, hbm, hbm],
        out_specs=(vmem, vmem),
        scratch_shapes=[
            pltpu.VMEM((whole, whole), BF16),
            pltpu.VMEM((own, whole), BF16),
            pltpu.VMEM((6,) + maps.shape, jnp.int32),
            pltpu.VMEM((own, 6 * face), BF16),
            pltpu.VMEM((6 * face, own), BF16),
            pltpu.VMEM((exchanges, 6, 2 * rhs, face), BF16),
            pltpu.VMEM((exchanges, 6, 2 * rhs, face), BF16),
            pltpu.VMEM((2 * rhs, whole), F32),
            pltpu.VMEM((rhs, own), F32),
            pltpu.VMEM((rhs, own), F32),
            pltpu.VMEM((ITERS, rhs, own), F32),
            pltpu.VMEM((ITERS, rhs, own), F32),
            pltpu.VMEM((ITERS, rhs, own), F32),
            pltpu.VMEM((rhs, own), F32),
            pltpu.VMEM((sums, rhs, 128), F32),
            pltpu.VMEM((sums, nx * ny, 1, 128), F32),
            pltpu.VMEM((sums, nz, 1, 128), F32),
            dma((3,)),
            dma((6,)),
            dma((6,)),
            dma((exchanges, 6)),
            dma((exchanges, 6)),
            dma((sums, nx * ny)),
            dma((sums, nx * ny)),
            dma((sums, nz)),
            dma((sums, nz)),
        ],
        compiler_params=pltpu.CompilerParams(
            collective_id=0, has_side_effects=True, vmem_limit_bytes=56 * 1024 * 1024
        ),
    )(target, maps, local_schur[0, 0, 0], inverse_rows[0, 0, 0])
    return (adjoint[None, None, None], ratio[0])


def solution(mesh):
    placed = P("gx", "gy", "gz", None, None)
    sizes = (mesh.shape["gx"], mesh.shape["gy"], mesh.shape["gz"])
    return jax.shard_map(
        functools.partial(local, sizes),
        mesh=mesh,
        in_specs=(placed, placed, placed, placed),
        out_specs=(placed, P()),
        check_vma=False,
    )
```
